32 devices in a mesh: py: 4 (over y, x), pz: 8 (over z, core).
Axes of the slice: x: 2, y: 2, z: 4, core: 2. Of those that a mesh axis runs over, the one named last changes fastest.
Arguments:
- positions: float32 [3, 131072], P(None, ('py', 'pz')), may hold values from 0 to 512, as said below
- masses: float32 [131072], P(('py', 'pz')), may hold values from 16 to 160
Outputs:
- forces: float32 [3, 32, 64, 512], P(None, 'py', 'pz')
The draws below stay inside these ranges and needn't reach their ends.
Inputs may be any that keep to these rules, and one draw needn't show every extreme that they name: `positions`: the particles come in blocks of 4096 columns; in the block numbered a 8 + b, row 0 lies in [a 8, (a + 1) * 8), row 1 in [b * 8, (b + 1) * 8), and row 2 in [0, 512).
All inputs are finite; a program needn't handle non-finite values.
Results may differ from the reference program's by a relative error of at most 0.0003.
Values sent between devices are 32-bit elements; how exact they have to be, the bound alone decides.
A program may use at most 64 MiB of HBM per device.

```python
import math
import jax
import jax.numpy as jnp

NX = 512
CY = 8
CZ = 8
PART_DEV = 4096
NY = 32
NZ = 64
NPART = 131072
N_PY = 4
N_PZ = 8


def draw_positions(key, part):
    total = PART_DEV * N_PY * N_PZ
    keys = jax.random.split(jax.random.fold_in(key, 17), 3)
    owner = jnp.arange(total, dtype=jnp.int32) // PART_DEV
    block_y = (owner // N_PZ).astype(jnp.float32)
    block_z = (owner % N_PZ).astype(jnp.float32)
    along_y = jax.random.uniform(keys[0], (total,), jnp.float32)
    along_z = jax.random.uniform(keys[1], (total,), jnp.float32)
    along_x = jax.random.uniform(keys[2], (total,), jnp.float32)
    coord_y = (block_y + along_y * 0.999) * CY
    coord_z = (block_z + along_z * 0.999) * CZ
    coord_x = along_x * (NX * 0.9999)
    return jnp.stack([coord_y, coord_z, coord_x]).astype(jnp.float32)


def level_of(key, extent, pieces, low, largest):
    gain = 1.0
    for position, parts in pieces:
        heights = jax.random.uniform(jax.random.fold_in(jax.random.fold_in(key, 6), position), (parts,), jnp.float32, low / len(pieces), largest / len(pieces))
        gain = gain * jnp.repeat(jnp.exp(heights), extent[position] // parts).reshape((-1,) + (1,) * (len(extent) - 1 - position))
    return gain


def setup_inputs(seed: int = 0) -> dict:
    key_list = jax.random.split(jax.random.key(seed), 3)
    return {
        "positions": draw_positions(jax.random.fold_in(key_list[2], 71), 0),
        "masses": jnp.clip(jnp.exp(math.log(160.0) - 2.3025851 * jax.random.uniform(key_list[1], (NPART,), jnp.float32) ** level_of(key_list[1], (NPART,), ((0, 32),), -0.2, 0.2)), 16.0, 160.0),
    }


smoothing_sq = 0.25


def wave_square(count, period):
    waves = jnp.arange(count, dtype=jnp.int32)
    folded = jnp.minimum(waves, period - waves).astype(jnp.float32)
    return (folded * (2.0 * math.pi / period)) ** 2


def reference(positions, masses):
    floors = jnp.floor(positions)
    fraction = positions - floors
    corner = floors.astype(jnp.int32)
    density = jnp.zeros((NY * NZ * NX,), jnp.float32)
    for offset_y in (0, 1):
        for offset_z in (0, 1):
            for offset_x in (0, 1):
                cell_y = (corner[0] + offset_y) % NY
                cell_z = (corner[1] + offset_z) % NZ
                cell_x = (corner[2] + offset_x) % NX
                weight_y = fraction[0] if offset_y else 1.0 - fraction[0]
                weight_z = fraction[1] if offset_z else 1.0 - fraction[1]
                weight_x = fraction[2] if offset_x else 1.0 - fraction[2]
                flat_index = (cell_y * NZ + cell_z) * NX + cell_x
                density = density.at[flat_index].add(masses * weight_y * weight_z * weight_x)
    density = density.reshape(NY, NZ, NX)
    total = wave_square(NY, NY)[:, None, None] + wave_square(NZ, NZ)[None, :, None] + wave_square(NX // 2 + 1, NX)[None, None, :]
    safe_total = jnp.where(total > 0, total, 1.0)
    green = jnp.where(total > 0, -4.0 * math.pi * jnp.exp(-smoothing_sq * total) / safe_total, 0.0)
    keep_x = jnp.arange(NX // 2 + 1, dtype=jnp.int32) < NX // 2
    green = jnp.where(keep_x[None, None, :], green, 0.0)
    spectrum = jnp.fft.rfftn(density)
    potential = jnp.fft.irfftn(spectrum * green, s=(NY, NZ, NX)).astype(jnp.float32)
    force_y = (jnp.roll(potential, 1, 0) - jnp.roll(potential, -1, 0)) * 0.5
    force_z = (jnp.roll(potential, 1, 1) - jnp.roll(potential, -1, 1)) * 0.5
    force_x = (jnp.roll(potential, 1, 2) - jnp.roll(potential, -1, 2)) * 0.5
    return jnp.stack([force_y, force_z, force_x])
```

```python
import functools
import math

import jax
import jax.numpy as jnp
import ml_dtypes
import numpy as np
from jax import lax
from jax.experimental import pallas as pl
from jax.experimental.pallas import tpu as pltpu
from jax.sharding import PartitionSpec as P

MESH = pl.DeviceIdType.MESH
F32 = jnp.float32
BF16 = jnp.bfloat16
SMOOTHING_SQ = 0.25
CELL = 8
PAIR = 2 * CELL
GROUPS = 128 // PAIR


def parts(table, count):
    out = []
    for _ in range(count):
        out.append(table.astype(ml_dtypes.bfloat16))
        table = table - out[-1].astype(np.float64)
    return np.stack(out)


def tables(n_py, n_pz, nx, nf):
    ny, nz = CELL * n_py, CELL * n_pz
    kept = nx // 2
    phase = (np.outer(np.arange(kept), np.arange(nx)) % nx) * (2 * np.pi / nx)
    line = np.concatenate([np.cos(phase), -np.sin(phase)])
    phase = (np.outer(np.arange(ny), np.arange(ny)) % ny) * (2 * np.pi / ny)
    eye = np.eye(nf)
    rows = np.concatenate([np.kron(np.cos(phase), eye), np.kron(np.sin(phase), eye)], axis=1)
    phase = (np.outer(np.arange(nz), np.arange(nz)) % nz) * (2 * np.pi / nz)
    cos, sin = np.cos(phase), np.sin(phase)
    forward = np.zeros((n_pz, 2, CELL, 2, nz))
    forward[:, 0, :, 0] = cos.reshape(n_pz, CELL, nz)
    forward[:, 0, :, 1] = -sin.reshape(n_pz, CELL, nz)
    forward[:, 1, :, 0] = sin.reshape(n_pz, CELL, nz)
    forward[:, 1, :, 1] = cos.reshape(n_pz, CELL, nz)
    forward = forward.reshape(2 * nz, 2, nz)
    turned = np.stack([forward[:, 1], -forward[:, 0]], axis=1)
    forward = np.concatenate([forward.reshape(2 * nz, 2 * nz), turned.reshape(2 * nz, 2 * nz)], 1)
    inverse = np.zeros((2, nz, n_pz, 2, CELL))
    inverse[0, :, :, 0] = cos.reshape(nz, n_pz, CELL)
    inverse[0, :, :, 1] = sin.reshape(nz, n_pz, CELL)
    inverse[1, :, :, 0] = -sin.reshape(nz, n_pz, CELL)
    inverse[1, :, :, 1] = cos.reshape(nz, n_pz, CELL)
    inverse = inverse.reshape(2 * nz, n_pz, 2, CELL)
    turned = np.stack([-inverse[:, :, 1], inverse[:, :, 0]], axis=2)
    inverse = np.concatenate([inverse.reshape(2 * nz, 2 * nz), turned.reshape(2 * nz, 2 * nz)], 1)
    return parts(line, 3), parts(rows, 3), parts(forward, 2), parts(inverse, 3)


def split(x, count=2):
    out = []
    for i in range(count):
        out.append(x.astype(BF16))
        if i < count - 1:
            x = x - out[-1].astype(F32)
    return out


def dot_parts(left, right, dims=((1,), (0,))):
    count = len(left)
    total = None
    for order in reversed(range(count)):
        for i in range(order + 1):
            term = lax.dot_general(
                left[i], right[order - i], (dims, ((), ())), preferred_element_type=F32
            )
            total = term if total is None else total + term
    return total


def swap_groups(tiles):
    group = lax.broadcasted_iota(jnp.int32, tiles[0].shape, 1) // PAIR
    moved = []
    for step in range(GROUPS):
        mixed = tiles[step]
        for a in range(1, GROUPS):
            mixed = jnp.where(group == a, tiles[(a + step) % GROUPS], mixed)
        moved.append(pltpu.roll(mixed, step * PAIR, 1) if step else mixed)
    out = []
    for a in range(GROUPS):
        mixed = moved[(0 - a) % GROUPS]
        for g in range(1, GROUPS):
            mixed = jnp.where(group == g, moved[(g - a) % GROUPS], mixed)
        out.append(mixed)
    return out


def green_factor(rank, n_py, n_pz, nx, nf):
    ny, nz = CELL * n_py, CELL * n_pz
    shape = (ny * nf, 2 * nz)
    row = lax.broadcasted_iota(jnp.int32, shape, 0)
    col = lax.broadcasted_iota(jnp.int32, shape, 1)

    def square(wave, period):
        folded = jnp.minimum(wave, period - wave).astype(F32)
        return (folded * (2.0 * math.pi / period)) ** 2

    wave_x = rank * nf + row % nf
    total = square(row // nf, ny) + square(col % nz, nz) + square(wave_x, nx)
    safe = jnp.where(total > 0, total, 1.0)
    green = jnp.where(total > 0, -4.0 * math.pi * jnp.exp(-SMOOTHING_SQ * total) / safe, 0.0)
    return green * (jnp.where(wave_x > 0, 2.0, 1.0) * (1.0 / float(ny * nz * nx)))


def kernel(
    n_py, n_pz, nx, nf, chunk,
    pos_hbm, mass_hbm, line_hbm, rows_hbm, fwd_hbm, inv_hbm,
    out_ref,
    pos_ref, mass_ref, line, rows, fwd, inv, table_sem,
    acc, halo_out, halo_in, halo_send, halo_recv,
    send1, recv1, field, send2, recv2, waves,
    send_sem1, recv_sem1, send_sem2, recv_sem2,
    edge_out, edge_in, edge_send, edge_recv,
):
    n = n_py * n_pz
    my_y, my_z = lax.axis_index("py"), lax.axis_index("pz")
    rank = my_y * n_pz + my_z

    loads = [
        pltpu.make_async_copy(src, dst, table_sem.at[i])
        for i, (src, dst) in enumerate(
            [
                (pos_hbm, pos_ref),
                (mass_hbm, mass_ref),
                (line_hbm, line),
                (rows_hbm, rows),
                (fwd_hbm, fwd),
                (inv_hbm, inv),
            ]
        )
    ]
    for load in loads:
        load.start()

    def coords(step):
        peer = lax.rem(rank + step, n)
        return peer, (peer // n_pz, lax.rem(peer, n_pz))

    barrier = pltpu.get_barrier_semaphore()

    @pl.loop(1, n)
    def _(step):
        pl.semaphore_signal(barrier, inc=1, device_id=coords(step)[1], device_id_type=MESH)

    base_y = (my_y * CELL).astype(F32)
    base_z = (my_z * CELL).astype(F32)
    acc[...] = jnp.zeros_like(acc)
    cell = lax.broadcasted_iota(jnp.int32, (CELL, chunk), 0).astype(F32)
    x_index = lax.broadcasted_iota(jnp.int32, (nx, chunk), 0).astype(F32)

    for load in loads[:2]:
        load.wait()

    @pl.loop(0, pos_ref.shape[1] // chunk)
    def _(turn):
        span = pl.ds(pl.multiple_of(turn * chunk, chunk), chunk)
        along_y = pos_ref[0:1, span] - base_y
        along_z = pos_ref[1:2, span] - base_z
        along_x = pos_ref[2:3, span]
        mass = mass_ref[0:1, span]
        floor_x = jnp.floor(along_x)
        frac_x = along_x - floor_x
        one_hot = jnp.where(x_index == floor_x, 1.0, 0.0).astype(BF16)
        hat_y = jnp.maximum(1.0 - jnp.abs(along_y - cell), 0.0)
        hat_z = jnp.maximum(1.0 - jnp.abs(along_z - cell), 0.0)
        last_y = jnp.maximum(along_y - (CELL - 1.0), 0.0)
        last_z = jnp.maximum(along_z - (CELL - 1.0), 0.0)
        highs, lows = [], []
        for share in (mass * (1.0 - frac_x), mass * frac_x):
            scaled = hat_z * share
            tiles = [hat_y[a : a + 1] * scaled for a in range(CELL)]
            tiles.append(last_y * scaled)
            tiles.append(hat_y * (last_z * share))
            tiles.append(jnp.where(cell == 0.0, last_y * (last_z * share), 0.0))
            high, low = split(jnp.concatenate(tiles, axis=0))
            highs.append(high)
            lows.append(low)
        stacked = jnp.concatenate(highs + lows, axis=0)
        acc[...] += lax.dot_general(
            stacked, one_hot, (((1,), (1,)), ((), ())), preferred_element_type=F32
        )

    plane = (CELL + 3) * CELL
    lower = acc[0:plane] + acc[2 * plane : 3 * plane]
    upper = acc[plane : 2 * plane] + acc[3 * plane : 4 * plane]
    grid = lower + pltpu.roll(upper, 1, 1)
    for i in range(3):
        halo_out[i] = grid[(CELL + i) * CELL : (CELL + i + 1) * CELL]

    up_y, up_z = lax.rem(my_y + 1, n_py), lax.rem(my_z + 1, n_pz)
    down_y, down_z = lax.rem(my_y + n_py - 1, n_py), lax.rem(my_z + n_pz - 1, n_pz)
    green = green_factor(rank, n_py, n_pz, nx, nf)
    pl.semaphore_wait(barrier, n - 1)
    halos = [
        pltpu.make_async_remote_copy(
            src_ref=halo_out.at[i],
            dst_ref=halo_in.at[i],
            send_sem=halo_send.at[i],
            recv_sem=halo_recv.at[i],
            device_id=target,
            device_id_type=MESH,
        )
        for i, target in enumerate([(up_y, my_z), (my_y, up_z), (up_y, up_z)])
    ]
    for halo in halos:
        halo.start()
    for load in loads[2:]:
        load.wait()
    for halo in halos:
        halo.wait()

    first = lax.broadcasted_iota(jnp.int32, (CELL, nx), 0) == 0
    beside = halo_in[1]
    doubled = []
    for a in range(CELL):
        tile = grid[a * CELL : (a + 1) * CELL]
        tile = tile + jnp.where(first, beside[a : a + 1], 0.0)
        if a == 0:
            tile = tile + halo_in[0] + jnp.where(first, halo_in[2], 0.0)
        doubled += [tile, tile]
    density = split(jnp.concatenate(doubled, axis=0))
    kept = nx // 2
    both = dot_parts([line[0], line[1]], density, ((1,), (1,)))
    is_real = lax.broadcasted_iota(jnp.int32, (kept, 2 * CELL * CELL), 1) // CELL % 2 == 0
    spectrum = jnp.where(is_real, both[:kept], both[kept:])
    for r in range(n):
        send1[r] = spectrum[r * nf : (r + 1) * nf]

    def exchange(source, target, send_sem, recv_sem):
        @pl.loop(1, n)
        def _(step):
            mirrored = n - step
            other_y = lax.rem(mirrored, n_py) ^ my_y
            other_z = (mirrored // n_py) ^ my_z
            peer, where = other_y * n_pz + other_z, (other_y, other_z)
            pltpu.make_async_remote_copy(
                src_ref=source.at[peer],
                dst_ref=target.at[rank],
                send_sem=send_sem,
                recv_sem=recv_sem,
                device_id=where,
                device_id_type=MESH,
            ).start()

        target[rank] = source[rank]
        others = pl.ds(0, n - 1)
        pltpu.make_async_copy(source.at[others], source.at[others], send_sem).wait()
        pltpu.make_async_copy(target.at[others], target.at[others], recv_sem).wait()

    exchange(send1, recv1, send_sem1, recv_sem1)

    for ay in range(n_py):
        for t in range(n_pz // GROUPS):
            tiles = [recv1[ay * n_pz + t * GROUPS + g] for g in range(GROUPS)]
            for a, tile in enumerate(swap_groups(tiles)):
                start = (ay * CELL + a) * nf
                field[start : start + nf, t * 128 : (t + 1) * 128] = tile
    width = 2 * CELL * n_pz

    def plane_transform(values, table):
        count = table.shape[0]
        along = dot_parts(split(values, count), [table[i] for i in range(count)])
        joined = jnp.concatenate([along[:, :width], along[:, width:]], axis=0)
        return dot_parts([rows[i] for i in range(count)], split(joined, count))

    values = field[...]
    row = lax.broadcasted_iota(jnp.int32, values.shape, 0)
    col = lax.broadcasted_iota(jnp.int32, values.shape, 1)
    constant = (row % nf + rank * nf == 0) & (col // CELL % 2 == 0)
    mean = jnp.sum(jnp.where(constant, values, 0.0), axis=0, keepdims=True)
    mean = jnp.sum(mean, axis=1, keepdims=True) * (1.0 / (CELL * CELL * n))
    values = values - jnp.where(constant, mean, 0.0)
    solved = plane_transform(plane_transform(values, fwd) * green, inv)
    for ay in range(n_py):
        for t in range(n_pz // GROUPS):
            tiles = []
            for a in range(CELL):
                start = (ay * CELL + a) * nf
                tiles.append(solved[start : start + nf, t * 128 : (t + 1) * 128])
            for g, tile in enumerate(swap_groups(tiles)):
                send2[ay * n_pz + t * GROUPS + g] = tile

    exchange(send2, recv2, send_sem2, recv_sem2)

    for r in range(n):
        waves[r * nf : (r + 1) * nf] = recv2[r]
    columns = split(jnp.transpose(waves[...]), 3)
    cosines = dot_parts(columns, [line[i, :kept] for i in range(3)])
    sines = dot_parts(columns, [line[i, kept:] for i in range(3)])
    potential = [
        cosines[a * PAIR : a * PAIR + CELL] + sines[a * PAIR + CELL : (a + 1) * PAIR]
        for a in range(CELL)
    ]
    edge_out[0] = potential[CELL - 1]
    edge_out[1] = potential[0]
    edge_out[2] = jnp.concatenate([tile[CELL - 1 : CELL] for tile in potential], axis=0)
    edge_out[3] = jnp.concatenate([tile[0:1] for tile in potential], axis=0)
    edges = [
        pltpu.make_async_remote_copy(
            src_ref=edge_out.at[i],
            dst_ref=edge_in.at[i],
            send_sem=edge_send.at[i],
            recv_sem=edge_recv.at[i],
            device_id=target,
            device_id_type=MESH,
        )
        for i, target in enumerate(
            [(up_y, my_z), (down_y, my_z), (my_y, up_z), (my_y, down_z)]
        )
    ]
    for edge in edges:
        edge.start()
    for a, tile in enumerate(potential):
        out_ref[2, a] = (pltpu.roll(tile, 1, 1) - pltpu.roll(tile, nx - 1, 1)) * 0.5
    for edge in edges:
        edge.wait()
    before, after = edge_in[2], edge_in[3]
    lane_row = lax.broadcasted_iota(jnp.int32, (CELL, nx), 0)
    for a, tile in enumerate(potential):
        below = potential[a - 1] if a else edge_in[0]
        above = potential[a + 1] if a < CELL - 1 else edge_in[1]
        out_ref[0, a] = (below - above) * 0.5
        lower = jnp.where(lane_row == 0, before[a : a + 1], pltpu.roll(tile, 1, 0))
        upper = jnp.where(lane_row == CELL - 1, after[a : a + 1], pltpu.roll(tile, CELL - 1, 0))
        out_ref[1, a] = (lower - upper) * 0.5


def solution(mesh):
    n_py, n_pz = mesh.shape["py"], mesh.shape["pz"]
    n = n_py * n_pz
    nx = 512
    nf = nx // 2 // n
    ny, nz = CELL * n_py, CELL * n_pz
    consts = tables(n_py, n_pz, nx, nf)

    def shards(positions, masses):
        chunk = min(positions.shape[1], 1024)
        vmem = pl.BlockSpec(memory_space=pltpu.VMEM)
        hbm = pl.BlockSpec(memory_space=pltpu.HBM)
        plane = (CELL + 3) * CELL
        block = pltpu.VMEM((n, nf, 128), F32)
        dma = pltpu.SemaphoreType.DMA
        return pl.pallas_call(
            functools.partial(kernel, n_py, n_pz, nx, nf, chunk),
            out_shape=jax.ShapeDtypeStruct((3, CELL, CELL, nx), F32),
            in_specs=[hbm] * 6,
            out_specs=vmem,
            scratch_shapes=[
                pltpu.VMEM(positions.shape, F32),
                pltpu.VMEM((1, positions.shape[1]), F32),
                *[pltpu.VMEM(table.shape, BF16) for table in consts],
                dma((6,)),
                pltpu.VMEM((4 * plane, nx), F32),
                pltpu.VMEM((3, CELL, nx), F32),
                pltpu.VMEM((3, CELL, nx), F32),
                dma((3,)),
                dma((3,)),
                block,
                block,
                pltpu.VMEM((ny * nf, 2 * nz), F32),
                block,
                block,
                pltpu.VMEM((n * nf, 128), F32),
                dma, dma, dma, dma,
                pltpu.VMEM((4, CELL, nx), F32),
                pltpu.VMEM((4, CELL, nx), F32),
                dma((4,)),
                dma((4,)),
            ],
            compiler_params=pltpu.CompilerParams(
                collective_id=0, has_side_effects=True, vmem_limit_bytes=67_043_328
            ),
        )(positions, masses.reshape(1, -1), *[jnp.asarray(table) for table in consts])

    return jax.shard_map(
        shards,
        mesh=mesh,
        in_specs=(P(None, ("py", "pz")), P(("py", "pz"))),
        out_specs=P(None, "py", "pz", None),
        check_vma=False,
    )
```

```python
import functools
import math

import jax
import jax.numpy as jnp
import ml_dtypes
import numpy as np
from jax import lax
from jax.experimental import pallas as pl
from jax.experimental.pallas import tpu as pltpu
from jax.sharding import PartitionSpec as P

MESH = pl.DeviceIdType.MESH
F32 = jnp.float32
BF16 = jnp.bfloat16
SMOOTHING_SQ = 0.25
CELL = 8
PAIR = 2 * CELL
GROUPS = 128 // PAIR


def parts(table, count):
    out = []
    for _ in range(count):
        out.append(table.astype(ml_dtypes.bfloat16))
        table = table - out[-1].astype(np.float64)
    return np.stack(out)


def tables(n_py, n_pz, nx, nf):
    ny, nz = CELL * n_py, CELL * n_pz
    kept = nx // 2
    phase = (np.outer(np.arange(kept), np.arange(nx)) % nx) * (2 * np.pi / nx)
    line = np.concatenate([np.cos(phase), -np.sin(phase)])
    phase = (np.outer(np.arange(ny), np.arange(ny)) % ny) * (2 * np.pi / ny)
    eye = np.eye(nf)
    rows = np.concatenate([np.kron(np.cos(phase), eye), np.kron(np.sin(phase), eye)], axis=1)
    phase = (np.outer(np.arange(nz), np.arange(nz)) % nz) * (2 * np.pi / nz)
    cos, sin = np.cos(phase), np.sin(phase)
    forward = np.zeros((n_pz, 2, CELL, 2, nz))
    forward[:, 0, :, 0] = cos.reshape(n_pz, CELL, nz)
    forward[:, 0, :, 1] = -sin.reshape(n_pz, CELL, nz)
    forward[:, 1, :, 0] = sin.reshape(n_pz, CELL, nz)
    forward[:, 1, :, 1] = cos.reshape(n_pz, CELL, nz)
    forward = forward.reshape(2 * nz, 2, nz)
    turned = np.stack([forward[:, 1], -forward[:, 0]], axis=1)
    forward = np.concatenate([forward.reshape(2 * nz, 2 * nz), turned.reshape(2 * nz, 2 * nz)], 1)
    inverse = np.zeros((2, nz, n_pz, 2, CELL))
    inverse[0, :, :, 0] = cos.reshape(nz, n_pz, CELL)
    inverse[0, :, :, 1] = sin.reshape(nz, n_pz, CELL)
    inverse[1, :, :, 0] = -sin.reshape(nz, n_pz, CELL)
    inverse[1, :, :, 1] = cos.reshape(nz, n_pz, CELL)
    inverse = inverse.reshape(2 * nz, n_pz, 2, CELL)
    turned = np.stack([-inverse[:, :, 1], inverse[:, :, 0]], axis=2)
    inverse = np.concatenate([inverse.reshape(2 * nz, 2 * nz), turned.reshape(2 * nz, 2 * nz)], 1)
    return parts(line, 3), parts(rows, 3), parts(forward, 2), parts(inverse, 3)


def split(x, count=2):
    out = []
    for i in range(count):
        out.append(x.astype(BF16))
        if i < count - 1:
            x = x - out[-1].astype(F32)
    return out


def dot_parts(left, right, dims=((1,), (0,))):
    count = len(left)
    total = None
    for order in reversed(range(count)):
        for i in range(order + 1):
            term = lax.dot_general(
                left[i], right[order - i], (dims, ((), ())), preferred_element_type=F32
            )
            total = term if total is None else total + term
    return total


def swap_groups(tiles):
    group = lax.broadcasted_iota(jnp.int32, tiles[0].shape, 1) // PAIR
    moved = []
    for step in range(GROUPS):
        mixed = tiles[step]
        for a in range(1, GROUPS):
            mixed = jnp.where(group == a, tiles[(a + step) % GROUPS], mixed)
        moved.append(pltpu.roll(mixed, step * PAIR, 1) if step else mixed)
    out = []
    for a in range(GROUPS):
        mixed = moved[(0 - a) % GROUPS]
        for g in range(1, GROUPS):
            mixed = jnp.where(group == g, moved[(g - a) % GROUPS], mixed)
        out.append(mixed)
    return out


def green_factor(rank, n_py, n_pz, nx, nf):
    ny, nz = CELL * n_py, CELL * n_pz
    shape = (ny * nf, 2 * nz)
    row = lax.broadcasted_iota(jnp.int32, shape, 0)
    col = lax.broadcasted_iota(jnp.int32, shape, 1)

    def square(wave, period):
        folded = jnp.minimum(wave, period - wave).astype(F32)
        return (folded * (2.0 * math.pi / period)) ** 2

    wave_x = rank * nf + row % nf
    total = square(row // nf, ny) + square(col % nz, nz) + square(wave_x, nx)
    safe = jnp.where(total > 0, total, 1.0)
    green = jnp.where(total > 0, -4.0 * math.pi * jnp.exp(-SMOOTHING_SQ * total) / safe, 0.0)
    return green * (jnp.where(wave_x > 0, 2.0, 1.0) * (1.0 / float(ny * nz * nx)))


def kernel(
    n_py, n_pz, nx, nf, chunk,
    pos_hbm, mass_hbm, line_hbm, rows_hbm, fwd_hbm, inv_hbm,
    out_ref,
    pos_ref, mass_ref, line, rows, fwd, inv, table_sem,
    hot, acc_halo, acc, halo_out, halo_in, halo_send, halo_recv,
    send1, recv1, field, send2, recv2, waves,
    send_sem1, recv_sem1, send_sem2, recv_sem2,
    edge_out, edge_in, edge_send, edge_recv,
):
    n = n_py * n_pz
    my_y, my_z = lax.axis_index("py"), lax.axis_index("pz")
    rank = my_y * n_pz + my_z

    loads = [
        pltpu.make_async_copy(src, dst, table_sem.at[i])
        for i, (src, dst) in enumerate(
            [
                (pos_hbm, pos_ref),
                (mass_hbm, mass_ref),
                (line_hbm, line),
                (rows_hbm, rows),
                (fwd_hbm, fwd),
                (inv_hbm, inv),
            ]
        )
    ]
    for load in loads:
        load.start()

    def coords(step):
        other_y = lax.rem(n - step, n_py) ^ my_y
        other_z = ((n - step) // n_py) ^ my_z
        return other_y * n_pz + other_z, (other_y, other_z)

    barrier = pltpu.get_barrier_semaphore()

    @pl.loop(1, n)
    def _(step):
        pl.semaphore_signal(barrier, inc=1, device_id=coords(step)[1], device_id_type=MESH)

    base_y = (my_y * CELL).astype(F32)
    base_z = (my_z * CELL).astype(F32)
    acc[...] = jnp.zeros_like(acc)
    acc_halo[...] = jnp.zeros_like(acc_halo)
    cell = lax.broadcasted_iota(jnp.int32, (CELL, chunk), 0).astype(F32)
    x_index = lax.broadcasted_iota(jnp.int32, (nx, chunk), 0).astype(F32)

    for load in loads[:2]:
        load.wait()

    def weights(turn):
        span = pl.ds(pl.multiple_of(turn * chunk, chunk), chunk)
        along_y = pos_ref[0:1, span] - base_y
        along_z = pos_ref[1:2, span] - base_z
        along_x = pos_ref[2:3, span]
        mass = mass_ref[0:1, span]
        floor_x = jnp.floor(along_x)
        frac_x = along_x - floor_x
        hat_y = jnp.maximum(1.0 - jnp.abs(along_y - cell), 0.0)
        hat_z = jnp.maximum(1.0 - jnp.abs(along_z - cell), 0.0)
        last_y = jnp.maximum(along_y - (CELL - 1.0), 0.0)
        last_z = jnp.maximum(along_z - (CELL - 1.0), 0.0)
        shares = (mass * (1.0 - frac_x), mass * frac_x)
        return span, floor_x, hat_y, hat_z, last_y, last_z, shares

    def deposited(tile_sets, one_hot):
        pairs = [split(jnp.concatenate(tiles, axis=0)) for tiles in tile_sets]
        stacked = jnp.concatenate([pair[i] for i in range(2) for pair in pairs], axis=0)
        return lax.dot_general(
            stacked, one_hot, (((1,), (1,)), ((), ())), preferred_element_type=F32
        )

    def settled(sums):
        plane = sums.shape[0] // 4
        lower = sums[0:plane] + sums[2 * plane : 3 * plane]
        upper = sums[plane : 2 * plane] + sums[3 * plane : 4 * plane]
        return lower + pltpu.roll(upper, 1, 1)

    turns = pos_ref.shape[1] // chunk

    @pl.loop(0, turns)
    def _(turn):
        span, floor_x, hat_y, hat_z, last_y, last_z, shares = weights(turn)
        one_hot = jnp.where(x_index == floor_x, 1.0, 0.0).astype(BF16)
        hot[:, span] = one_hot
        tile_sets = [
            [
                last_y * (hat_z * share),
                hat_y * (last_z * share),
                jnp.where(cell == 0.0, last_y * (last_z * share), 0.0),
            ]
            for share in shares
        ]
        acc_halo[...] += deposited(tile_sets, one_hot)

    outer = settled(acc_halo[...])
    for i in range(3):
        halo_out[i] = outer[i * CELL : (i + 1) * CELL]

    up_y, up_z = lax.rem(my_y + 1, n_py), lax.rem(my_z + 1, n_pz)
    down_y, down_z = lax.rem(my_y + n_py - 1, n_py), lax.rem(my_z + n_pz - 1, n_pz)
    pl.semaphore_wait(barrier, n - 1)
    halos = [
        pltpu.make_async_remote_copy(
            src_ref=halo_out.at[i],
            dst_ref=halo_in.at[i],
            send_sem=halo_send.at[i],
            recv_sem=halo_recv.at[i],
            device_id=target,
            device_id_type=MESH,
        )
        for i, target in enumerate([(up_y, my_z), (my_y, up_z), (up_y, up_z)])
    ]
    for halo in halos:
        halo.start()

    @pl.loop(0, turns)
    def _(turn):
        span, _, hat_y, hat_z, _, _, shares = weights(turn)
        tile_sets = []
        for share in shares:
            scaled = hat_z * share
            tile_sets.append([hat_y[a : a + 1] * scaled for a in range(CELL)])
        acc[...] += deposited(tile_sets, hot[:, span])

    grid = settled(acc[...])
    green = green_factor(rank, n_py, n_pz, nx, nf)
    for load in loads[2:]:
        load.wait()
    for halo in halos:
        halo.wait()

    first = lax.broadcasted_iota(jnp.int32, (CELL, nx), 0) == 0
    beside = halo_in[1]
    doubled = []
    for a in range(CELL):
        tile = grid[a * CELL : (a + 1) * CELL]
        tile = tile + jnp.where(first, beside[a : a + 1], 0.0)
        if a == 0:
            tile = tile + halo_in[0] + jnp.where(first, halo_in[2], 0.0)
        doubled += [tile, tile]
    density = split(jnp.concatenate(doubled, axis=0))
    kept = nx // 2
    both = dot_parts([line[0], line[1]], density, ((1,), (1,)))
    is_real = lax.broadcasted_iota(jnp.int32, (kept, 2 * CELL * CELL), 1) // CELL % 2 == 0
    spectrum = jnp.where(is_real, both[:kept], both[kept:])
    for r in range(n):
        send1[r] = spectrum[r * nf : (r + 1) * nf]

    def exchange(source, target, send_sem, recv_sem):
        @pl.loop(1, n)
        def _(step):
            peer, where = coords(step)
            pltpu.make_async_remote_copy(
                src_ref=source.at[peer],
                dst_ref=target.at[rank],
                send_sem=send_sem,
                recv_sem=recv_sem,
                device_id=where,
                device_id_type=MESH,
            ).start()

        target[rank] = source[rank]
        others = pl.ds(0, n - 1)
        pltpu.make_async_copy(source.at[others], source.at[others], send_sem).wait()
        pltpu.make_async_copy(target.at[others], target.at[others], recv_sem).wait()

    exchange(send1, recv1, send_sem1, recv_sem1)

    for ay in range(n_py):
        for t in range(n_pz // GROUPS):
            tiles = [recv1[ay * n_pz + t * GROUPS + g] for g in range(GROUPS)]
            for a, tile in enumerate(swap_groups(tiles)):
                start = (ay * CELL + a) * nf
                field[start : start + nf, t * 128 : (t + 1) * 128] = tile
    width = 2 * CELL * n_pz

    def plane_transform(values, table):
        count = table.shape[0]
        along = dot_parts(split(values, count), [table[i] for i in range(count)])
        joined = jnp.concatenate([along[:, :width], along[:, width:]], axis=0)
        return dot_parts([rows[i] for i in range(count)], split(joined, count))

    values = field[...]
    row = lax.broadcasted_iota(jnp.int32, values.shape, 0)
    col = lax.broadcasted_iota(jnp.int32, values.shape, 1)
    constant = (row % nf + rank * nf == 0) & (col // CELL % 2 == 0)
    mean = jnp.sum(jnp.where(constant, values, 0.0), axis=0, keepdims=True)
    mean = jnp.sum(mean, axis=1, keepdims=True) * (1.0 / (CELL * CELL * n))
    values = values - jnp.where(constant, mean, 0.0)
    solved = plane_transform(plane_transform(values, fwd) * green, inv)
    for ay in range(n_py):
        for t in range(n_pz // GROUPS):
            tiles = []
            for a in range(CELL):
                start = (ay * CELL + a) * nf
                tiles.append(solved[start : start + nf, t * 128 : (t + 1) * 128])
            for g, tile in enumerate(swap_groups(tiles)):
                send2[ay * n_pz + t * GROUPS + g] = tile

    exchange(send2, recv2, send_sem2, recv_sem2)

    for r in range(n):
        waves[r * nf : (r + 1) * nf] = recv2[r]
    columns = split(jnp.transpose(waves[...]), 3)
    cosines = dot_parts(columns, [line[i, :kept] for i in range(3)])
    sines = dot_parts(columns, [line[i, kept:] for i in range(3)])
    potential = [
        cosines[a * PAIR : a * PAIR + CELL] + sines[a * PAIR + CELL : (a + 1) * PAIR]
        for a in range(CELL)
    ]
    edge_out[0] = potential[CELL - 1]
    edge_out[1] = potential[0]
    edge_out[2] = jnp.concatenate([tile[CELL - 1 : CELL] for tile in potential], axis=0)
    edge_out[3] = jnp.concatenate([tile[0:1] for tile in potential], axis=0)
    edges = [
        pltpu.make_async_remote_copy(
            src_ref=edge_out.at[i],
            dst_ref=edge_in.at[i],
            send_sem=edge_send.at[i],
            recv_sem=edge_recv.at[i],
            device_id=target,
            device_id_type=MESH,
        )
        for i, target in enumerate(
            [(up_y, my_z), (down_y, my_z), (my_y, up_z), (my_y, down_z)]
        )
    ]
    for edge in edges:
        edge.start()
    for a, tile in enumerate(potential):
        out_ref[2, a] = (pltpu.roll(tile, 1, 1) - pltpu.roll(tile, nx - 1, 1)) * 0.5
    for edge in edges:
        edge.wait()
    before, after = edge_in[2], edge_in[3]
    lane_row = lax.broadcasted_iota(jnp.int32, (CELL, nx), 0)
    for a, tile in enumerate(potential):
        below = potential[a - 1] if a else edge_in[0]
        above = potential[a + 1] if a < CELL - 1 else edge_in[1]
        out_ref[0, a] = (below - above) * 0.5
        lower = jnp.where(lane_row == 0, before[a : a + 1], pltpu.roll(tile, 1, 0))
        upper = jnp.where(lane_row == CELL - 1, after[a : a + 1], pltpu.roll(tile, CELL - 1, 0))
        out_ref[1, a] = (lower - upper) * 0.5


def solution(mesh):
    n_py, n_pz = mesh.shape["py"], mesh.shape["pz"]
    n = n_py * n_pz
    nx = 512
    nf = nx // 2 // n
    ny, nz = CELL * n_py, CELL * n_pz
    consts = tables(n_py, n_pz, nx, nf)

    def shards(positions, masses):
        chunk = min(positions.shape[1], 2048)
        vmem = pl.BlockSpec(memory_space=pltpu.VMEM)
        hbm = pl.BlockSpec(memory_space=pltpu.HBM)
        block = pltpu.VMEM((n, nf, 128), F32)
        dma = pltpu.SemaphoreType.DMA
        return pl.pallas_call(
            functools.partial(kernel, n_py, n_pz, nx, nf, chunk),
            out_shape=jax.ShapeDtypeStruct((3, CELL, CELL, nx), F32),
            in_specs=[hbm] * 6,
            out_specs=vmem,
            scratch_shapes=[
                pltpu.VMEM(positions.shape, F32),
                pltpu.VMEM((1, positions.shape[1]), F32),
                *[pltpu.VMEM(table.shape, BF16) for table in consts],
                dma((6,)),
                pltpu.VMEM((nx, positions.shape[1]), BF16),
                pltpu.VMEM((4 * 3 * CELL, nx), F32),
                pltpu.VMEM((4 * CELL * CELL, nx), F32),
                pltpu.VMEM((3, CELL, nx), F32),
                pltpu.VMEM((3, CELL, nx), F32),
                dma((3,)),
                dma((3,)),
                block,
                block,
                pltpu.VMEM((ny * nf, 2 * nz), F32),
                block,
                block,
                pltpu.VMEM((n * nf, 128), F32),
                dma, dma, dma, dma,
                pltpu.VMEM((4, CELL, nx), F32),
                pltpu.VMEM((4, CELL, nx), F32),
                dma((4,)),
                dma((4,)),
            ],
            compiler_params=pltpu.CompilerParams(
                collective_id=0, has_side_effects=True, vmem_limit_bytes=67_043_328
            ),
        )(positions, masses.reshape(1, -1), *[jnp.asarray(table) for table in consts])

    return jax.shard_map(
        shards,
        mesh=mesh,
        in_specs=(P(None, ("py", "pz")), P(("py", "pz"))),
        out_specs=P(None, "py", "pz", None),
        check_vma=False,
    )
```
